32 devices in a mesh: rep: 2 (over x), dp: 16 (over y, z, core).
Axes of the slice: x: 2, y: 2, z: 4, core: 2. Of those that a mesh axis runs over, the one named last changes fastest.
Arguments:
- x: bfloat16 [32, 2048, 896], P(('rep', 'dp')), parts along dimension 0
- dy: bfloat16 [32, 2048, 896], P(('rep', 'dp')), parts along dimension 0
- w_gate: bfloat16 [2, 896, 2560], replicated
- w_up: bfloat16 [2, 896, 2560], replicated
- w_down: bfloat16 [2, 2560, 896], replicated
- m_w_gate: float32 [2, 896, 2560], replicated
- m_w_up: float32 [2, 896, 2560], replicated
- m_w_down: float32 [2, 2560, 896], replicated
- v_w_gate: float32 [2, 896, 2560], replicated
- v_w_up: float32 [2, 896, 2560], replicated
- v_w_down: float32 [2, 2560, 896], replicated
Outputs:
- output 1: bfloat16 [4, 896, 2560], P('rep'), parts along dimension 0
- output 2: bfloat16 [4, 896, 2560], P('rep'), parts along dimension 0
- output 3: bfloat16 [4, 2560, 896], P('rep'), parts along dimension 0
- output 4: float32 [4, 896, 2560], P('rep'), parts along dimension 0
- output 5: float32 [4, 896, 2560], P('rep'), parts along dimension 0
- output 6: float32 [4, 2560, 896], P('rep'), parts along dimension 0
- output 7: float32 [4, 896, 2560], P('rep'), parts along dimension 0
- output 8: float32 [4, 896, 2560], P('rep'), parts along dimension 0
- output 9: float32 [4, 2560, 896], P('rep'), parts along dimension 0
There are 2 independent parts. The reference program is written for one: setup_inputs(seed, part) draws one part's arguments, and reference() takes and returns one part's arrays. A program takes and returns all parts, laid end to end along the dimension named above; an argument that names none is the same for every part.
All inputs are finite; a program needn't handle non-finite values.
Results may differ from the reference program's by a relative error of at most 0.022.
Values are sent between devices in bfloat16 or wider.
A program may use at most 2.5 GiB of HBM per device.

```python
import jax
import jax.numpy as jnp
from jax import lax

SEQUENCES = 16
TOKENS = 2048
D = 896
FF = 2560
LAYERS = 2
NAMES = ("w_gate", "w_up", "w_down")
SHAPES = {"w_gate": (LAYERS, D, FF), "w_up": (LAYERS, D, FF), "w_down": (LAYERS, FF, D)}


def bump(key, n, height):
    away = (jnp.arange(n, dtype=jnp.int32) - jax.random.randint(key, (), 0, n, jnp.int32)) % n
    return jnp.where(away < n // 8, height, 1.0)


def together(key, own, strength):
    shared = jax.random.normal(key, own.shape[1:], jnp.float32)
    return (own + strength * shared) * lax.rsqrt(1 + strength * strength)


def setup_inputs(seed: int = 0, part: int = 0) -> dict:
    kx, kdy, ka, kb, kz, kf, kh, kl, *keys = jax.random.split(jax.random.key(seed), 8 + 3 * len(NAMES))
    kx, kdy, ka, kb = (jax.random.fold_in(k, part) for k in (kx, kdy, ka, kb))
    kw, km, kv = (keys[i::3] for i in range(3))
    shape = (SEQUENCES, TOKENS, D)
    much_x, much_dy = jax.random.uniform(kz, (2,), jnp.float32, 0.0, 1.0)
    loud = 2.0 ** jax.random.uniform(jax.random.fold_in(kz, 1), (), jnp.float32, -1.0, 2.0)
    layers = 2.0 ** jax.random.uniform(kl, (LAYERS, 1, 1), jnp.float32, -1.0, 1.0)
    x = together(ka, jax.random.normal(kx, shape, jnp.float32), much_x) * bump(kf, D, 4.0)
    dy = together(kb, jax.random.normal(kdy, shape, jnp.float32), much_dy)
    drawn = {"x": x.astype(jnp.bfloat16), "dy": (loud * dy * (SEQUENCES * TOKENS) ** -0.5).astype(jnp.bfloat16)}
    for key, name in zip(kw, NAMES, strict=True):
        w = jax.random.normal(key, SHAPES[name], jnp.float32) * SHAPES[name][1] ** -0.5
        drawn[name] = (w * {"w_gate": 1.0, "w_up": bump(kh, FF, 4.0), "w_down": layers}[name]).astype(jnp.bfloat16)
    for key, name in zip(km, NAMES, strict=True):
        drawn[f"m_{name}"] = 0.1 * jax.random.normal(key, SHAPES[name], jnp.float32)
    for key, name in zip(kv, NAMES, strict=True):
        drawn[f"v_{name}"] = jax.random.uniform(key, SHAPES[name], jnp.float32, 0.005, 0.015)
    return drawn


def matmul(a, w):
    return jnp.dot(a, w, preferred_element_type=jnp.float32).astype(jnp.bfloat16)


def normed(h):
    wide = h.astype(jnp.float32)
    scale = lax.rsqrt(jnp.mean(wide**2, -1, keepdims=True) + 1e-6)
    return (wide * scale).astype(jnp.bfloat16)


def layer(h, w):
    a = normed(h)
    gate = jnp.dot(a, w["w_gate"], preferred_element_type=jnp.float32)
    up = jnp.dot(a, w["w_up"], preferred_element_type=jnp.float32)
    return h + matmul((jax.nn.silu(gate) * up).astype(jnp.bfloat16), w["w_down"])


def adamw(w, m, v, g):
    m = 0.9 * m + 0.1 * g
    v = 0.95 * v + 0.05 * g * g
    step = m * lax.rsqrt(v + 1e-8) + 0.1 * w
    return (w - 0.02 * step).astype(jnp.bfloat16), m, v


def stack(weights, h):
    return lax.scan(lambda h, w: (layer(h, w), None), h, weights)[0]


def reference(x, dy, w_gate, w_up, w_down, m_w_gate, m_w_up, m_w_down, v_w_gate, v_w_up, v_w_down):
    weights = dict(zip(NAMES, (w_gate, w_up, w_down), strict=True))

    def take(so_far, sequence):
        h, by_y = sequence
        _, back = jax.vjp(lambda w: stack(w, h), weights)
        return jax.tree.map(lambda total, term: total + term.astype(jnp.float32), so_far, back(by_y)[0]), None

    none_yet = {name: jnp.zeros(w.shape, jnp.float32) for name, w in weights.items()}
    by_weights, _ = lax.scan(take, none_yet, (x, dy))
    gradients = [by_weights[name].astype(jnp.bfloat16).astype(jnp.float32) for name in NAMES]
    new = [
        adamw(w.astype(jnp.float32), m, v, g)
        for w, m, v, g in zip((w_gate, w_up, w_down), (m_w_gate, m_w_up, m_w_down), (v_w_gate, v_w_up, v_w_down), gradients, strict=True)
    ]
    return tuple(one[which] for which in range(3) for one in new)
```

```python
import functools

import jax
import jax.numpy as jnp
from jax import lax
from jax.experimental import pallas as pl
from jax.experimental.pallas import tpu as pltpu
from jax.sharding import PartitionSpec as P

MESH = pl.DeviceIdType.MESH
F32, BF16 = jnp.float32, jnp.bfloat16
TOKENS, D, FF = 2048, 896, 2560
BLOCK = 256
PER_LAYER = FF // BLOCK
BLOCKS = 2 * PER_LAYER
TILE = 512
HALF, QUARTER = D // 2, D // 4
LANES = 128
SLOTS_A = {1: 2, 2: 2, 3: 4, 4: 2, 5: 4, 6: 2, 7: 2}
SLOTS_B = {1: 2, 2: 6, 3: 2, 4: 2, 5: 2, 6: 6, 7: 2}


def nt(a, b):
    return lax.dot_general(a, b, (((1,), (1,)), ((), ())), preferred_element_type=F32)


def nn(a, b):
    return jnp.dot(a, b, preferred_element_type=F32)


def rows(start, size):
    return pl.ds(pl.multiple_of(start, 32), size)


def scale_of(wide):
    return lax.rsqrt(jnp.mean(wide * wide, -1, keepdims=True) + 1e-6)


def step_kernel(x_hbm, dy_hbm, wg_hbm, wu_hbm, wd_hbm, ga, gb, P_, H, DY, AT, DT, ACC, HID, DG, DU, wg_v, wu_v, wd_v, *comm):
    (sb_a, keep_a, r1_a, s2_a, k2_a, r2_a, s3_a, acc_a, r3_a, s4_a, r4_a, g_a,
     sb_b, keep_b, r1_b, s2_b, acc1_b, r2_b, s3_b, k2_b, r3_b, s4_b, r4_b, g_b,
     load_sem, w_sem, loc_a, loc_b, send_a, send_b, *recvs) = comm
    recv_a = dict(zip(range(1, 8), recvs[:7], strict=True))
    recv_b = dict(zip(range(1, 8), recvs[7:], strict=True))
    me = lax.axis_index("dp")
    c = me % 2
    z = (me // 2) % 4
    y = me // 8
    odd = z % 2
    high = z // 2
    inner = (odd + high) == 1
    end = (odd + high) != 1
    to_core = me + 1 - 2 * c
    to_y = me + 8 - 16 * y
    to_z = me + 2 - 4 * odd
    to_mid = me + 2 - 4 * high

    def remote(src, dst, send, recv, to):
        return pltpu.make_async_remote_copy(
            src_ref=src, dst_ref=dst, send_sem=send, recv_sem=recv, device_id={"dp": to}, device_id_type=MESH
        )

    barrier = pltpu.get_barrier_semaphore()
    for to in (to_core, to_y, to_z):
        pl.semaphore_signal(barrier, inc=1, device_id={"dp": to}, device_id_type=MESH)

    @pl.when(inner)
    def _():
        pl.semaphore_signal(barrier, inc=1, device_id={"dp": to_mid}, device_id_type=MESH)
        pl.semaphore_wait(barrier, 4)

    @pl.when(end)
    def _():
        pl.semaphore_wait(barrier, 3)

    def weight_copies(i):
        layer, j, slot = (i // PER_LAYER) % 2, i % PER_LAYER, i % 2
        cols = pl.ds(pl.multiple_of(j * BLOCK, BLOCK), BLOCK)
        return (
            pltpu.make_async_copy(wg_hbm.at[layer, :, cols], wg_v.at[slot], w_sem.at[slot, 0]),
            pltpu.make_async_copy(wu_hbm.at[layer, :, cols], wu_v.at[slot], w_sem.at[slot, 1]),
            pltpu.make_async_copy(wd_hbm.at[layer, cols, :], wd_v.at[slot], w_sem.at[slot, 2]),
        )

    def fetch(i):
        for copy in weight_copies(i):
            copy.start()

    def arrive(i):
        for copy in weight_copies(i):
            copy.wait()

    fetch(0)
    load_x = pltpu.make_async_copy(x_hbm.at[0], H, load_sem.at[0])
    load_dy = pltpu.make_async_copy(dy_hbm.at[0], DY, load_sem.at[1])
    load_x.start()
    load_dy.start()
    load_x.wait()

    def tiles(body, tile=TILE):
        def one(k, carry):
            body(pl.ds(pl.multiple_of(k * tile, tile), tile))
            return carry

        lax.fori_loop(0, TOKENS // tile, one, 0)

    def norm_into(source):
        def body(at):
            wide = source[at, :].astype(F32)
            P_[at, :] = (wide * scale_of(wide)).astype(BF16)
            ACC[at, :] = jnp.zeros((128, D), F32)

        tiles(body, 128)

    def flip(source, target):
        def body(at):
            target[:, at] = source[at, :].T

        tiles(body, 256)

    norm_into(H)

    def forward(i, carry):
        slot = i % 2
        arrive(i)
        fetch(i + 1)

        def body(at):
            a = P_[at, :]
            gate, up = nn(a, wg_v[slot]), nn(a, wu_v[slot])
            hid = (gate * jax.nn.sigmoid(gate) * up).astype(BF16)
            ACC[at, :] += nn(hid, wd_v[slot])

        tiles(body)
        return carry

    lax.fori_loop(0, PER_LAYER, forward, 0)

    def join(at):
        h = (H[at, :].astype(F32) + ACC[at, :].astype(BF16).astype(F32)).astype(BF16)
        H[at, :] = h

    tiles(join, 128)
    norm_into(H)
    load_dy.wait()
    flip(P_, AT)
    flip(DY, DT)

    def own_a(b):
        return ga.at[b, :, rows(c * HALF + y * QUARTER, QUARTER), :]

    def other_a(b):
        return ga.at[b, :, rows(c * HALF + (1 - y) * QUARTER, QUARTER), :]

    def core_of(g, b, which):
        return g.at[b, :, rows(which * HALF, HALF), :]

    def own_b(b):
        return gb.at[b, :, rows(c * HALF + high * QUARTER, QUARTER), :]

    def other_b(b):
        return gb.at[b, :, rows(c * HALF + (1 - high) * QUARTER, QUARTER), :]

    def live(t, s):
        return (t - s >= 0) & (t - s < BLOCKS)

    def a_copy(s, b, src, dst, to):
        return remote(src, dst, send_a.at[s], recv_a[s].at[b % SLOTS_A[s]], to)

    def b_copy(s, b, src, dst, to):
        return remote(src, dst, send_b.at[s], recv_b[s].at[b % SLOTS_B[s]], to)

    def tick_a(t):
        @pl.when(live(t, 7))
        def _():
            b = t - 7
            a_copy(7, b, core_of(ga, b, c), core_of(ga, b, c), to_core).wait_send()
            a_copy(7, b, core_of(ga, b, 1 - c), core_of(ga, b, 1 - c), to_core).wait_recv()

        @pl.when(live(t, 6))
        def _():
            b = t - 6
            a_copy(6, b, own_a(b), own_a(b), to_y).wait_send()
            a_copy(6, b, other_a(b), other_a(b), to_y).wait_recv()
            a_copy(7, b, core_of(ga, b, c), core_of(ga, b, c), to_core).start()

        @pl.when(live(t, 5))
        def _():
            b = t - 5

            @pl.when(inner)
            def _():
                a_copy(5, b, g_a, own_a(b), to_z).wait_send()
                pltpu.make_async_copy(g_a, own_a(b), loc_a).wait()

            @pl.when(end)
            def _():
                a_copy(5, b, g_a, own_a(b), to_z).wait_recv()

            a_copy(6, b, own_a(b), own_a(b), to_y).start()

        @pl.when(live(t, 4) & inner)
        def _():
            b = t - 4
            copy = a_copy(4, b, s4_a, r4_a.at[b % 2], to_mid)
            copy.wait_send()
            copy.wait_recv()
            g_a[...] = (s4_a[...].astype(F32) + r4_a[b % 2].astype(F32)).astype(BF16)
            pltpu.make_async_copy(g_a, own_a(b), loc_a).start()
            a_copy(5, b, g_a, own_a(b), to_z).start()

        @pl.when(live(t, 3))
        def _():
            b = t - 3
            slot = b % SLOTS_A[3]
            copy = a_copy(3, b, s3_a, r3_a.at[slot], to_z)

            @pl.when(end)
            def _():
                copy.wait_send()

            @pl.when(inner)
            def _():
                copy.wait_recv()
                s4_a[...] = (acc_a[...] + r3_a[slot].astype(F32)).astype(BF16)
                a_copy(4, b, s4_a, r4_a.at[b % 2], to_mid).start()

        @pl.when(live(t, 2))
        def _():
            b = t - 2
            copy = a_copy(2, b, s2_a, r2_a.at[b % 2], to_y)
            copy.wait_send()
            copy.wait_recv()
            total = k2_a[...] + r2_a[b % 2].astype(F32)

            @pl.when(inner)
            def _():
                acc_a[...] = total

            @pl.when(end)
            def _():
                s3_a[...] = total.astype(BF16)
                a_copy(3, b, s3_a, r3_a.at[b % SLOTS_A[3]], to_z).start()

        @pl.when(live(t, 1))
        def _():
            b = t - 1
            slot = b % 2
            copy = a_copy(1, b, sb_a.at[slot], r1_a.at[slot], to_core)
            copy.wait_send()
            copy.wait_recv()
            mine, theirs = rows(y * QUARTER, QUARTER), rows((1 - y) * QUARTER, QUARTER)
            k2_a[...] = keep_a[slot, :, mine, :] + r1_a[slot, :, mine, :].astype(F32)
            s2_a[...] = (keep_a[slot, :, theirs, :] + r1_a[slot, :, theirs, :].astype(F32)).astype(BF16)
            a_copy(2, b, s2_a, r2_a.at[slot], to_y).start()

        @pl.when(live(t, 0))
        def _():
            a_copy(1, t, sb_a.at[t % 2], r1_a.at[t % 2], to_core).start()

    def tick_b(t):
        @pl.when(live(t, 7))
        def _():
            b = t - 7
            b_copy(7, b, core_of(gb, b, c), core_of(gb, b, c), to_core).wait_send()
            b_copy(7, b, core_of(gb, b, 1 - c), core_of(gb, b, 1 - c), to_core).wait_recv()

        @pl.when(live(t, 6))
        def _():
            b = t - 6
            copy = b_copy(6, b, core_of(gb, b, c), core_of(gb, b, c), to_z)

            @pl.when(inner)
            def _():
                copy.wait_send()

            @pl.when(end)
            def _():
                copy.wait_recv()

            b_copy(7, b, core_of(gb, b, c), core_of(gb, b, c), to_core).start()

        @pl.when(live(t, 5) & inner)
        def _():
            b = t - 5
            b_copy(5, b, g_b, own_b(b), to_mid).wait_send()
            b_copy(5, b, g_b, other_b(b), to_mid).wait_recv()
            pltpu.make_async_copy(g_b, own_b(b), loc_b).wait()
            b_copy(6, b, core_of(gb, b, c), core_of(gb, b, c), to_z).start()

        @pl.when(live(t, 4) & inner)
        def _():
            b = t - 4
            copy = b_copy(4, b, s4_b, r4_b.at[b % 2], to_y)
            copy.wait_send()
            copy.wait_recv()
            g_b[...] = (s4_b[...].astype(F32) + r4_b[b % 2].astype(F32)).astype(BF16)
            pltpu.make_async_copy(g_b, own_b(b), loc_b).start()
            b_copy(5, b, g_b, own_b(b), to_mid).start()

        @pl.when(live(t, 3) & inner)
        def _():
            b = t - 3
            copy = b_copy(3, b, s3_b, r3_b.at[b % 2], to_mid)
            copy.wait_send()
            copy.wait_recv()
            s4_b[...] = (k2_b[...] + r3_b[b % 2].astype(F32)).astype(BF16)
            b_copy(4, b, s4_b, r4_b.at[b % 2], to_y).start()

        @pl.when(live(t, 2))
        def _():
            b = t - 2
            slot = b % SLOTS_B[2]
            copy = b_copy(2, b, s2_b, r2_b.at[slot], to_z)

            @pl.when(end)
            def _():
                copy.wait_send()

            @pl.when(inner)
            def _():
                copy.wait_recv()
                mine, theirs = rows(high * QUARTER, QUARTER), rows((1 - high) * QUARTER, QUARTER)
                k2_b[...] = acc1_b[:, mine, :] + r2_b[slot, :, mine, :].astype(F32)
                s3_b[...] = (acc1_b[:, theirs, :] + r2_b[slot, :, theirs, :].astype(F32)).astype(BF16)
                b_copy(3, b, s3_b, r3_b.at[b % 2], to_mid).start()

        @pl.when(live(t, 1))
        def _():
            b = t - 1
            slot = b % 2
            copy = b_copy(1, b, sb_b.at[slot], r1_b.at[slot], to_core)
            copy.wait_send()
            copy.wait_recv()
            total = keep_b[slot] + r1_b[slot].astype(F32)

            @pl.when(inner)
            def _():
                acc1_b[...] = total

            @pl.when(end)
            def _():
                s2_b[...] = total.astype(BF16)
                b_copy(2, b, s2_b, r2_b.at[b % SLOTS_B[2]], to_z).start()

        @pl.when(live(t, 0))
        def _():
            b_copy(1, t, sb_b.at[t % 2], r1_b.at[t % 2], to_core).start()

    def turn():
        load = pltpu.make_async_copy(x_hbm.at[0], P_, load_sem.at[0])
        load.start()

        def body(at):
            wide = H[at, :].astype(F32)
            scale = scale_of(wide)
            da = ACC[at, :].astype(BF16).astype(F32)
            along = jnp.sum(da * wide, -1, keepdims=True) * (scale * scale * scale) * (1.0 / D)
            by_h = (da * scale - wide * along).astype(BF16).astype(F32)
            DY[at, :] = (DY[at, :].astype(F32) + by_h).astype(BF16)

        tiles(body, 128)
        flip(DY, DT)
        load.wait()
        norm_into(P_)
        flip(P_, AT)

    def gradients(t):
        slot = (t + PER_LAYER) % 2

        def body(at):
            a = P_[at, :]
            gate, up = nn(a, wg_v[slot]), nn(a, wu_v[slot])
            by_hid = nt(DY[at, :], wd_v[slot]).astype(BF16).astype(F32)
            sig = jax.nn.sigmoid(gate)
            act = gate * sig
            HID[at, :] = (act * up).astype(BF16)
            by_gate = (by_hid * up * (sig + act * (1.0 - sig))).astype(BF16)
            by_up = (by_hid * act).astype(BF16)
            DG[at, :] = by_gate
            DU[at, :] = by_up

        tiles(body)

        @pl.when(t < PER_LAYER)
        def _():
            def body(at):
                ACC[at, :] += nt(DG[at, :], wg_v[slot]) + nt(DU[at, :], wu_v[slot])

            tiles(body)

    def weights_of(t):
        slot = t % 2
        for m, (left, right) in enumerate(((AT, DG), (AT, DU), (DT, HID))):
            total = nn(left[rows((1 - c) * HALF, HALF), :], right[...]).astype(BF16)
            sb_a[slot, m] = total[:, :LANES]
            sb_b[slot, m] = total[:, LANES:]
            total = nn(left[rows(c * HALF, HALF), :], right[...])
            keep_a[slot, m] = total[:, :LANES]
            keep_b[slot, m] = total[:, LANES:]

    def main(t, carry):
        @pl.when(t == PER_LAYER)
        def _():
            turn()

        @pl.when(t < BLOCKS)
        def _():
            arrive(t + PER_LAYER)

            @pl.when(t < BLOCKS - 1)
            def _():
                fetch(t + PER_LAYER + 1)

            gradients(t)

        tick_b(t - 1)

        @pl.when(t < BLOCKS)
        def _():
            weights_of(t)

        tick_a(t)
        return carry

    lax.fori_loop(0, BLOCKS + 8, main, 0)


def summed_gradients(x, dy, wg, wu, wd):
    unit = lambda n, height, dtype: pltpu.VMEM((n, 3, height, LANES) if n else (3, height, LANES), dtype)
    scratch = [
        pltpu.VMEM((TOKENS, D), BF16),
        pltpu.VMEM((TOKENS, D), BF16),
        pltpu.VMEM((TOKENS, D), BF16),
        pltpu.VMEM((D, TOKENS), BF16),
        pltpu.VMEM((D, TOKENS), BF16),
        pltpu.VMEM((TOKENS, D), F32),
        pltpu.VMEM((TOKENS, BLOCK), BF16),
        pltpu.VMEM((TOKENS, BLOCK), BF16),
        pltpu.VMEM((TOKENS, BLOCK), BF16),
        pltpu.VMEM((2, D, BLOCK), BF16),
        pltpu.VMEM((2, D, BLOCK), BF16),
        pltpu.VMEM((2, BLOCK, D), BF16),
        unit(2, HALF, BF16), unit(2, HALF, F32), unit(2, HALF, BF16),
        unit(0, QUARTER, BF16), unit(0, QUARTER, F32), unit(2, QUARTER, BF16),
        unit(0, QUARTER, BF16), unit(0, QUARTER, F32), unit(SLOTS_A[3], QUARTER, BF16),
        unit(0, QUARTER, BF16), unit(2, QUARTER, BF16), unit(0, QUARTER, BF16),
        unit(2, HALF, BF16), unit(2, HALF, F32), unit(2, HALF, BF16),
        unit(0, HALF, BF16), unit(0, HALF, F32), unit(SLOTS_B[2], HALF, BF16),
        unit(0, QUARTER, BF16), unit(0, QUARTER, F32), unit(2, QUARTER, BF16),
        unit(0, QUARTER, BF16), unit(2, QUARTER, BF16), unit(0, QUARTER, BF16),
        pltpu.SemaphoreType.DMA((2,)),
        pltpu.SemaphoreType.DMA((2, 3)),
        pltpu.SemaphoreType.DMA,
        pltpu.SemaphoreType.DMA,
        pltpu.SemaphoreType.DMA((8,)),
        pltpu.SemaphoreType.DMA((8,)),
        *[pltpu.SemaphoreType.DMA((SLOTS_A[s],)) for s in range(1, 8)],
        *[pltpu.SemaphoreType.DMA((SLOTS_B[s],)) for s in range(1, 8)],
    ]
    out = jax.ShapeDtypeStruct((BLOCKS, 3, D, LANES), BF16)
    return pl.pallas_call(
        step_kernel,
        out_shape=(out, out),
        in_specs=[pl.BlockSpec(memory_space=pl.ANY)] * 5,
        out_specs=(pl.BlockSpec(memory_space=pl.ANY),) * 2,
        scratch_shapes=scratch,
        compiler_params=pltpu.CompilerParams(collective_id=0, has_side_effects=True, vmem_limit_bytes=62 * 2**20),
        name="gradients",
    )(x, dy, wg, wu, wd)


def adamw(w, m, v, g):
    m = 0.9 * m + 0.1 * g
    v = 0.95 * v + 0.05 * g * g
    step = m * lax.rsqrt(v + 1e-8) + 0.1 * w
    return (w - 0.02 * step).astype(BF16), m, v


def update_wide(w_ref, m_ref, v_ref, ga_ref, gb_ref, w_out, m_out, v_out):
    for j in range(FF // LANES):
        at = slice(j * LANES, (j + 1) * LANES)
        g = (ga_ref, gb_ref)[j % 2][j // 2, 0].astype(F32)
        w_out[0, :, at], m_out[0, :, at], v_out[0, :, at] = adamw(
            w_ref[0, :, at].astype(F32), m_ref[0, :, at], v_ref[0, :, at], g
        )


def update_tall(w_ref, m_ref, v_ref, ga_ref, gb_ref, w_out, m_out, v_out):
    for k, g_ref in enumerate((ga_ref, gb_ref)):
        at = slice(k * LANES, (k + 1) * LANES)
        g = g_ref[0, 0].T.astype(F32)
        w_out[0, at], m_out[0, at], v_out[0, at] = adamw(w_ref[0, at].astype(F32), m_ref[0, at], v_ref[0, at], g)


def update(which, w, m, v, ga, gb):
    if which < 2:
        height = 112
        kernel, grid = update_wide, (2, D // height)
        spec = pl.BlockSpec((1, height, FF), lambda l, i: (l, i, 0))
        g_spec = pl.BlockSpec((PER_LAYER, 1, height, LANES), lambda l, i: (1 - l, which, i, 0))
    else:
        kernel, grid = update_tall, (2, PER_LAYER)
        spec = pl.BlockSpec((1, BLOCK, D), lambda l, i: (l, i, 0))
        g_spec = pl.BlockSpec((1, 1, D, LANES), lambda l, i: ((1 - l) * PER_LAYER + i, which, 0, 0))
    return pl.pallas_call(
        kernel,
        grid=grid,
        in_specs=[spec] * 3 + [g_spec] * 2,
        out_specs=[spec] * 3,
        out_shape=[jax.ShapeDtypeStruct(w.shape, t) for t in (BF16, F32, F32)],
        compiler_params=pltpu.CompilerParams(vmem_limit_bytes=48 * 2**20),
        name=f"update_{which}",
    )(w, m, v, ga, gb)


def solution(mesh):
    def step(x, dy, *arrays):
        weights, m, v = (arrays[i : i + 3] for i in (0, 3, 6))
        ga, gb = summed_gradients(x, dy, *weights)
        new = [update(i, weights[i], m[i], v[i], ga, gb) for i in range(3)]
        return tuple(one[which] for which in range(3) for one in new)

    return jax.shard_map(
        step,
        mesh=mesh,
        in_specs=(P(("rep", "dp"), None, None),) * 2 + (P(None, None, None),) * 9,
        out_specs=(P("rep", None, None),) * 9,
        check_vma=False,
    )
```

```python
import jax
import jax.numpy as jnp
from jax import lax
from jax.experimental import pallas as pl
from jax.experimental.pallas import tpu as pltpu
from jax.sharding import PartitionSpec as P

MESH = pl.DeviceIdType.MESH
F32, BF16 = jnp.float32, jnp.bfloat16
TOKENS, D, FF = 2048, 896, 2560
BLOCK = 256
PER_LAYER = FF // BLOCK
BLOCKS = 2 * PER_LAYER
TILE = 512
HALF, QUARTER = D // 2, D // 4
LANES = 128
SLOTS_A = {2: 2, 3: 4, 4: 2, 5: 4, 6: 2, 7: 2}
SLOTS_B = {2: 6, 3: 2, 4: 2, 5: 2, 6: 6, 7: 2}


def nt(a, b):
    return lax.dot_general(a, b, (((1,), (1,)), ((), ())), preferred_element_type=F32)


def nn(a, b):
    return jnp.dot(a, b, preferred_element_type=F32)


def rows(start, size):
    return pl.ds(pl.multiple_of(start, 32), size)


def scale_of(wide):
    return lax.rsqrt(jnp.mean(wide * wide, -1, keepdims=True) + 1e-6)


def step_kernel(x_hbm, dy_hbm, wg_hbm, wu_hbm, wd_hbm, ga, gb, P_, H, DY, AT, DT, ACC, HID, DG, DU, wg_v, wu_v, wd_v, *comm):
    (sb_a, keep_a, r1_a, s2_a, k2_a, r2_a, s3_a, acc_a, r3_a, s4_a, r4_a, g_a,
     sb_b, keep_b, r1_b, s2_b, acc1_b, r2_b, s3_b, k2_b, r3_b, s4_b, r4_b, g_b,
     load_sem, w_sem, loc_a, loc_b, first_send, first_recv, send_a, send_b, *recvs) = comm
    recv_a = dict(zip(range(2, 8), recvs[:6], strict=True))
    recv_b = dict(zip(range(2, 8), recvs[6:], strict=True))
    me = lax.axis_index("dp")
    c = me % 2
    z = (me // 2) % 4
    y = me // 8
    odd = z % 2
    high = z // 2
    inner = (odd + high) == 1
    end = (odd + high) != 1
    to_core = me + 1 - 2 * c
    to_y = me + 8 - 16 * y
    to_z = me + 2 - 4 * odd
    to_mid = me + 2 - 4 * high

    def remote(src, dst, send, recv, to):
        return pltpu.make_async_remote_copy(
            src_ref=src, dst_ref=dst, send_sem=send, recv_sem=recv, device_id={"dp": to}, device_id_type=MESH
        )

    barrier = pltpu.get_barrier_semaphore()
    for to in (to_core, to_y, to_z):
        pl.semaphore_signal(barrier, inc=1, device_id={"dp": to}, device_id_type=MESH)

    @pl.when(inner)
    def _():
        pl.semaphore_signal(barrier, inc=1, device_id={"dp": to_mid}, device_id_type=MESH)
        pl.semaphore_wait(barrier, 4)

    @pl.when(end)
    def _():
        pl.semaphore_wait(barrier, 3)

    def weight_copies(i):
        layer, j, slot = (i // PER_LAYER) % 2, i % PER_LAYER, i % 2
        cols = pl.ds(pl.multiple_of(j * BLOCK, BLOCK), BLOCK)
        return (
            pltpu.make_async_copy(wg_hbm.at[layer, :, cols], wg_v.at[slot], w_sem.at[slot, 0]),
            pltpu.make_async_copy(wu_hbm.at[layer, :, cols], wu_v.at[slot], w_sem.at[slot, 1]),
            pltpu.make_async_copy(wd_hbm.at[layer, cols, :], wd_v.at[slot], w_sem.at[slot, 2]),
        )

    def fetch(i):
        for copy in weight_copies(i):
            copy.start()

    def arrive(i):
        for copy in weight_copies(i):
            copy.wait()

    fetch(0)
    loads = [
        pltpu.make_async_copy(x_hbm.at[0, k * TILE : (k + 1) * TILE], H.at[k * TILE : (k + 1) * TILE], load_sem.at[k])
        for k in range(TOKENS // TILE)
    ]
    load_dy = pltpu.make_async_copy(dy_hbm.at[0], DY, load_sem.at[TOKENS // TILE])
    for load in loads:
        load.start()
    load_dy.start()

    def tiles(body):
        for k in range(TOKENS // TILE):
            body(slice(k * TILE, (k + 1) * TILE))

    def normed(h):
        wide = h.astype(F32)
        return (wide * scale_of(wide)).astype(BF16)

    def down_of(a, slot):
        gate, up = nn(a, wg_v[slot]), nn(a, wu_v[slot])
        return nn((gate * jax.nn.sigmoid(gate) * up).astype(BF16), wd_v[slot])

    def flip_a_share(i):
        for k in range(TOKENS // TILE):
            q = pl.ds(pl.multiple_of((i * (TOKENS // TILE) + k) * LANES, LANES), LANES)
            AT[0, :, q] = P_[0, q, :].T
            DT[:, q] = DY[q, :].T

    def first(at):
        a = normed(H[at, :])
        P_[0, at, :] = a
        ACC[at, :] = down_of(a, 0)

    def last(at):
        total = ACC[at, :] + down_of(P_[0, at, :], (PER_LAYER - 1) % 2)
        h = (H[at, :].astype(F32) + total.astype(BF16).astype(F32)).astype(BF16)
        H[at, :] = h
        a = normed(h)
        P_[1, at, :] = a
        AT[1, :, at] = a.T
        ACC[at, :] = jnp.zeros((TILE, D), F32)

    def forward(i, flips):
        slot = i % 2
        arrive(i)
        fetch(i + 1)

        def body(at):
            ACC[at, :] += down_of(P_[0, at, :], slot)

        tiles(body)
        if flips:
            flip_a_share(i - 1)

    arrive(0)
    fetch(1)
    for k, load in enumerate(loads):
        load.wait()
        first(slice(k * TILE, (k + 1) * TILE))
    load_dy.wait()
    with_flips = 1 + TILE // LANES

    @pl.loop(1, with_flips)
    def _(i):
        forward(i, True)

    @pl.loop(with_flips, PER_LAYER - 1)
    def _(i):
        forward(i, False)

    arrive(PER_LAYER - 1)
    fetch(PER_LAYER)
    tiles(last)

    def own_a(b):
        return ga.at[b, :, rows(c * HALF + y * QUARTER, QUARTER), :]

    def other_a(b):
        return ga.at[b, :, rows(c * HALF + (1 - y) * QUARTER, QUARTER), :]

    def core_of(g, b, which):
        return g.at[b, :, rows(which * HALF, HALF), :]

    def own_b(b):
        return gb.at[b, :, rows(c * HALF + high * QUARTER, QUARTER), :]

    def other_b(b):
        return gb.at[b, :, rows(c * HALF + (1 - high) * QUARTER, QUARTER), :]

    def live(t, s):
        return (t - s >= 0) & (t - s < BLOCKS)

    def a_copy(s, b, src, dst, to):
        return remote(src, dst, send_a.at[s], recv_a[s].at[b % SLOTS_A[s]], to)

    def b_copy(s, b, src, dst, to):
        return remote(src, dst, send_b.at[s], recv_b[s].at[b % SLOTS_B[s]], to)

    def first_a(b, m):
        slot = b % 2
        return remote(sb_a.at[slot, m], r1_a.at[slot, m], first_send.at[0, slot, m], first_recv.at[0, slot, m], to_core)

    def first_b(b, m):
        slot = b % 2
        return remote(sb_b.at[slot, m], r1_b.at[slot, m], first_send.at[1, slot, m], first_recv.at[1, slot, m], to_core)

    def tick_a(t):
        @pl.when(live(t, 6))
        def _():
            b = t - 6
            a_copy(7, b, core_of(ga, b, c), core_of(ga, b, c), to_core).wait_send()
            a_copy(7, b, core_of(ga, b, 1 - c), core_of(ga, b, 1 - c), to_core).wait_recv()

        @pl.when(live(t, 5))
        def _():
            b = t - 5
            a_copy(6, b, own_a(b), own_a(b), to_y).wait_send()
            a_copy(6, b, other_a(b), other_a(b), to_y).wait_recv()
            a_copy(7, b, core_of(ga, b, c), core_of(ga, b, c), to_core).start()

        @pl.when(live(t, 4))
        def _():
            b = t - 4

            @pl.when(inner)
            def _():
                a_copy(5, b, g_a, own_a(b), to_z).wait_send()
                pltpu.make_async_copy(g_a, own_a(b), loc_a).wait()

            @pl.when(end)
            def _():
                a_copy(5, b, g_a, own_a(b), to_z).wait_recv()

            a_copy(6, b, own_a(b), own_a(b), to_y).start()

        @pl.when(live(t, 3) & inner)
        def _():
            b = t - 3
            copy = a_copy(4, b, s4_a, r4_a.at[b % 2], to_mid)
            copy.wait_send()
            copy.wait_recv()
            g_a[...] = (s4_a[...].astype(F32) + r4_a[b % 2].astype(F32)).astype(BF16)
            pltpu.make_async_copy(g_a, own_a(b), loc_a).start()
            a_copy(5, b, g_a, own_a(b), to_z).start()

        @pl.when(live(t, 2))
        def _():
            b = t - 2
            slot = b % SLOTS_A[3]
            copy = a_copy(3, b, s3_a, r3_a.at[slot], to_z)

            @pl.when(end)
            def _():
                copy.wait_send()

            @pl.when(inner)
            def _():
                copy.wait_recv()
                s4_a[...] = (acc_a[...] + r3_a[slot].astype(F32)).astype(BF16)
                a_copy(4, b, s4_a, r4_a.at[b % 2], to_mid).start()

        @pl.when(live(t, 1))
        def _():
            b = t - 1
            copy = a_copy(2, b, s2_a, r2_a.at[b % 2], to_y)
            copy.wait_send()
            copy.wait_recv()
            total = k2_a[...] + r2_a[b % 2].astype(F32)

            @pl.when(inner)
            def _():
                acc_a[...] = total

            @pl.when(end)
            def _():
                s3_a[...] = total.astype(BF16)
                a_copy(3, b, s3_a, r3_a.at[b % SLOTS_A[3]], to_z).start()

        @pl.when(live(t, 0))
        def _():
            b = t
            slot = b % 2
            for m in range(3):
                first_a(b, m).wait()
            mine, theirs = rows(y * QUARTER, QUARTER), rows((1 - y) * QUARTER, QUARTER)
            k2_a[...] = keep_a[slot, :, mine, :] + r1_a[slot, :, mine, :].astype(F32)
            s2_a[...] = (keep_a[slot, :, theirs, :] + r1_a[slot, :, theirs, :].astype(F32)).astype(BF16)
            a_copy(2, b, s2_a, r2_a.at[slot], to_y).start()

    def tick_b(t):
        @pl.when(live(t, 6))
        def _():
            b = t - 6
            b_copy(7, b, core_of(gb, b, c), core_of(gb, b, c), to_core).wait_send()
            b_copy(7, b, core_of(gb, b, 1 - c), core_of(gb, b, 1 - c), to_core).wait_recv()

        @pl.when(live(t, 5))
        def _():
            b = t - 5
            copy = b_copy(6, b, core_of(gb, b, c), core_of(gb, b, c), to_z)

            @pl.when(inner)
            def _():
                copy.wait_send()

            @pl.when(end)
            def _():
                copy.wait_recv()

            b_copy(7, b, core_of(gb, b, c), core_of(gb, b, c), to_core).start()

        @pl.when(live(t, 4) & inner)
        def _():
            b = t - 4
            b_copy(5, b, g_b, own_b(b), to_mid).wait_send()
            b_copy(5, b, g_b, other_b(b), to_mid).wait_recv()
            pltpu.make_async_copy(g_b, own_b(b), loc_b).wait()
            b_copy(6, b, core_of(gb, b, c), core_of(gb, b, c), to_z).start()

        @pl.when(live(t, 3) & inner)
        def _():
            b = t - 3
            copy = b_copy(4, b, s4_b, r4_b.at[b % 2], to_y)
            copy.wait_send()
            copy.wait_recv()
            g_b[...] = (s4_b[...].astype(F32) + r4_b[b % 2].astype(F32)).astype(BF16)
            pltpu.make_async_copy(g_b, own_b(b), loc_b).start()
            b_copy(5, b, g_b, own_b(b), to_mid).start()

        @pl.when(live(t, 2) & inner)
        def _():
            b = t - 2
            copy = b_copy(3, b, s3_b, r3_b.at[b % 2], to_mid)
            copy.wait_send()
            copy.wait_recv()
            s4_b[...] = (k2_b[...] + r3_b[b % 2].astype(F32)).astype(BF16)
            b_copy(4, b, s4_b, r4_b.at[b % 2], to_y).start()

        @pl.when(live(t, 1))
        def _():
            b = t - 1
            slot = b % SLOTS_B[2]
            copy = b_copy(2, b, s2_b, r2_b.at[slot], to_z)

            @pl.when(end)
            def _():
                copy.wait_send()

            @pl.when(inner)
            def _():
                copy.wait_recv()
                mine, theirs = rows(high * QUARTER, QUARTER), rows((1 - high) * QUARTER, QUARTER)
                k2_b[...] = acc1_b[:, mine, :] + r2_b[slot, :, mine, :].astype(F32)
                s3_b[...] = (acc1_b[:, theirs, :] + r2_b[slot, :, theirs, :].astype(F32)).astype(BF16)
                b_copy(3, b, s3_b, r3_b.at[b % 2], to_mid).start()

        @pl.when(live(t, 0))
        def _():
            b = t
            slot = b % 2
            for m in range(3):
                first_b(b, m).wait()
            total = keep_b[slot] + r1_b[slot].astype(F32)

            @pl.when(inner)
            def _():
                acc1_b[...] = total

            @pl.when(end)
            def _():
                s2_b[...] = total.astype(BF16)
                b_copy(2, b, s2_b, r2_b.at[b % SLOTS_B[2]], to_z).start()

    def turn(at, by_a):
        wide = H[at, :].astype(F32)
        scale = scale_of(wide)
        da = by_a.astype(BF16).astype(F32)
        along = jnp.sum(da * wide, -1, keepdims=True) * (scale * scale * scale) * (1.0 / D)
        by_h = (da * scale - wide * along).astype(BF16).astype(F32)
        by_y = (DY[at, :].astype(F32) + by_h).astype(BF16)
        DY[at, :] = by_y
        DT[:, at] = by_y.T

    def gradients(t):
        slot = (t + PER_LAYER) % 2
        layer = 1 - t // PER_LAYER

        def body(at):
            a = P_[layer, at, :]
            gate, up = nn(a, wg_v[slot]), nn(a, wu_v[slot])
            by_hid = nt(DY[at, :], wd_v[slot]).astype(BF16).astype(F32)
            sig = jax.nn.sigmoid(gate)
            act = gate * sig
            HID[at, :] = (act * up).astype(BF16)
            by_gate = (by_hid * up * (sig + act * (1.0 - sig))).astype(BF16)
            by_up = (by_hid * act).astype(BF16)
            DG[at, :] = by_gate
            DU[at, :] = by_up

        tiles(body)

    def by_input(t, then=None):
        slot = (t + PER_LAYER) % 2

        def body(at):
            total = ACC[at, :] + (nt(DG[at, :], wg_v[slot]) + nt(DU[at, :], wu_v[slot]))
            if then is None:
                ACC[at, :] = total
            else:
                then(at, total)

        tiles(body)

    def weights_of(t):
        slot = t % 2
        layer = 1 - t // PER_LAYER
        pairs = ((AT.at[layer], DG), (AT.at[layer], DU), (DT, HID))

        def send(m):
            first_a(t, m).start()
            first_b(t, m).start()

        for m, (left, right) in enumerate(pairs):
            total = nn(left[rows((1 - c) * HALF, HALF), :], right[...]).astype(BF16)
            sb_a[slot, m] = total[:, :LANES]
            sb_b[slot, m] = total[:, LANES:]
            if m:
                send(m - 1)
        for m, (left, right) in enumerate(pairs):
            total = nn(left[rows(c * HALF, HALF), :], right[...])
            keep_a[slot, m] = total[:, :LANES]
            keep_b[slot, m] = total[:, LANES:]
            if m == 0:
                send(2)

    def main(t, carry):
        @pl.when(t < BLOCKS)
        def _():
            arrive(t + PER_LAYER)

            @pl.when(t < BLOCKS - 1)
            def _():
                fetch(t + PER_LAYER + 1)

            gradients(t)

        tick_b(t - 1)

        @pl.when(t < BLOCKS)
        def _():
            weights_of(t)

        @pl.when(t < PER_LAYER - 1)
        def _():
            by_input(t)

        @pl.when(t == PER_LAYER - 1)
        def _():
            by_input(t, turn)

        tick_a(t)
        return carry

    lax.fori_loop(0, BLOCKS + 7, main, 0)


def summed_gradients(x, dy, wg, wu, wd):
    unit = lambda n, height, dtype: pltpu.VMEM((n, 3, height, LANES) if n else (3, height, LANES), dtype)
    scratch = [
        pltpu.VMEM((2, TOKENS, D), BF16),
        pltpu.VMEM((TOKENS, D), BF16),
        pltpu.VMEM((TOKENS, D), BF16),
        pltpu.VMEM((2, D, TOKENS), BF16),
        pltpu.VMEM((D, TOKENS), BF16),
        pltpu.VMEM((TOKENS, D), F32),
        pltpu.VMEM((TOKENS, BLOCK), BF16),
        pltpu.VMEM((TOKENS, BLOCK), BF16),
        pltpu.VMEM((TOKENS, BLOCK), BF16),
        pltpu.VMEM((2, D, BLOCK), BF16),
        pltpu.VMEM((2, D, BLOCK), BF16),
        pltpu.VMEM((2, BLOCK, D), BF16),
        unit(2, HALF, BF16), unit(2, HALF, F32), unit(2, HALF, BF16),
        unit(0, QUARTER, BF16), unit(0, QUARTER, F32), unit(2, QUARTER, BF16),
        unit(0, QUARTER, BF16), unit(0, QUARTER, F32), unit(SLOTS_A[3], QUARTER, BF16),
        unit(0, QUARTER, BF16), unit(2, QUARTER, BF16), unit(0, QUARTER, BF16),
        unit(2, HALF, BF16), unit(2, HALF, F32), unit(2, HALF, BF16),
        unit(0, HALF, BF16), unit(0, HALF, F32), unit(SLOTS_B[2], HALF, BF16),
        unit(0, QUARTER, BF16), unit(0, QUARTER, F32), unit(2, QUARTER, BF16),
        unit(0, QUARTER, BF16), unit(2, QUARTER, BF16), unit(0, QUARTER, BF16),
        pltpu.SemaphoreType.DMA((TOKENS // TILE + 1,)),
        pltpu.SemaphoreType.DMA((2, 3)),
        pltpu.SemaphoreType.DMA,
        pltpu.SemaphoreType.DMA,
        pltpu.SemaphoreType.DMA((2, 2, 3)),
        pltpu.SemaphoreType.DMA((2, 2, 3)),
        pltpu.SemaphoreType.DMA((8,)),
        pltpu.SemaphoreType.DMA((8,)),
        *[pltpu.SemaphoreType.DMA((SLOTS_A[s],)) for s in range(2, 8)],
        *[pltpu.SemaphoreType.DMA((SLOTS_B[s],)) for s in range(2, 8)],
    ]
    out = jax.ShapeDtypeStruct((BLOCKS, 3, D, LANES), BF16)
    return pl.pallas_call(
        step_kernel,
        out_shape=(out, out),
        in_specs=[pl.BlockSpec(memory_space=pl.ANY)] * 5,
        out_specs=(pl.BlockSpec(memory_space=pl.ANY),) * 2,
        scratch_shapes=scratch,
        compiler_params=pltpu.CompilerParams(collective_id=0, has_side_effects=True, vmem_limit_bytes=62 * 2**20),
        name="gradients",
    )(x, dy, wg, wu, wd)


def adamw(w, m, v, g):
    m = 0.9 * m + 0.1 * g
    v = 0.95 * v + 0.05 * g * g
    step = m * lax.rsqrt(v + 1e-8) + 0.1 * w
    return (w - 0.02 * step).astype(BF16), m, v


def update_wide(*refs):
    ins, outs = (refs[:5], refs[5:10]), (refs[10:13], refs[13:])
    for (w_ref, m_ref, v_ref, ga_ref, gb_ref), (w_out, m_out, v_out) in zip(ins, outs, strict=True):
        for j in range(FF // LANES):
            at = slice(j * LANES, (j + 1) * LANES)
            g = (ga_ref, gb_ref)[j % 2][j // 2, 0].astype(F32)
            w_out[0, :, at], m_out[0, :, at], v_out[0, :, at] = adamw(
                w_ref[0, :, at].astype(F32), m_ref[0, :, at], v_ref[0, :, at], g
            )


TALL = 2 * BLOCK


def update_tall(w_ref, m_ref, v_ref, ga_ref, gb_ref, w_out, m_out, v_out):
    for k in range(TALL // LANES):
        at = slice(k * LANES, (k + 1) * LANES)
        g = (ga_ref, gb_ref)[k % 2][k // 2, 0].T.astype(F32)
        w_out[0, at], m_out[0, at], v_out[0, at] = adamw(w_ref[0, at].astype(F32), m_ref[0, at], v_ref[0, at], g)


def new_arrays(shape):
    return [jax.ShapeDtypeStruct(shape, t) for t in (BF16, F32, F32)]


def update_gate_up(gate, up, ga, gb):
    height = 112
    spec = pl.BlockSpec((1, height, FF), lambda l, i: (l, i, 0))

    def g_spec(which):
        return pl.BlockSpec((PER_LAYER, 1, height, LANES), lambda l, i: (1 - l, which, i, 0))

    new = pl.pallas_call(
        update_wide,
        grid=(2, D // height),
        in_specs=[spec] * 3 + [g_spec(0)] * 2 + [spec] * 3 + [g_spec(1)] * 2,
        out_specs=[spec] * 6,
        out_shape=new_arrays(gate[0].shape) * 2,
        compiler_params=pltpu.CompilerParams(vmem_limit_bytes=60 * 2**20),
        name="update_gate_up",
    )(*gate, ga, gb, *up, ga, gb)
    return new[:3], new[3:]


def update_down(down, ga, gb):
    spec = pl.BlockSpec((1, TALL, D), lambda l, i: (l, i, 0))
    g_spec = pl.BlockSpec((TALL // BLOCK, 1, D, LANES), lambda l, i: ((1 - l) * (FF // TALL) + i, 2, 0, 0))
    return pl.pallas_call(
        update_tall,
        grid=(2, FF // TALL),
        in_specs=[spec] * 3 + [g_spec] * 2,
        out_specs=[spec] * 3,
        out_shape=new_arrays(down[0].shape),
        compiler_params=pltpu.CompilerParams(vmem_limit_bytes=60 * 2**20),
        name="update_down",
    )(*down, ga, gb)


def solution(mesh):
    def step(x, dy, *arrays):
        weights, m, v = (arrays[i : i + 3] for i in (0, 3, 6))
        ga, gb = summed_gradients(x, dy, *weights)
        gate, up, down = zip(weights, m, v, strict=True)
        new = [*update_gate_up(gate, up, ga, gb), update_down(down, ga, gb)]
        return tuple(one[which] for which in range(3) for one in new)

    return jax.shard_map(
        step,
        mesh=mesh,
        in_specs=(P(("rep", "dp"), None, None),) * 2 + (P(None, None, None),) * 9,
        out_specs=(P("rep", None, None),) * 9,
        check_vma=False,
    )
```

```python
import jax
import jax.numpy as jnp
from jax import lax
from jax.experimental import pallas as pl
from jax.experimental.pallas import tpu as pltpu
from jax.sharding import PartitionSpec as P

MESH = pl.DeviceIdType.MESH
F32, BF16 = jnp.float32, jnp.bfloat16
TOKENS, D, FF = 2048, 896, 2560
BLOCK = 256
PER_LAYER = FF // BLOCK
BLOCKS = 2 * PER_LAYER
TILE = 512
HALF, QUARTER = D // 2, D // 4
LANES = 128
SLOTS_A = {2: 2, 3: 4, 4: 2, 5: 4, 6: 2, 7: 2}
SLOTS_B = {2: 6, 3: 2, 4: 2, 5: 2, 6: 6, 7: 2}


def nt(a, b):
    return lax.dot_general(a, b, (((1,), (1,)), ((), ())), preferred_element_type=F32)


def nn(a, b):
    return jnp.dot(a, b, preferred_element_type=F32)


def rows(start, size):
    return pl.ds(pl.multiple_of(start, 32), size)


def scale_of(wide):
    return lax.rsqrt(jnp.mean(wide * wide, -1, keepdims=True) + 1e-6)


def step_kernel(x_hbm, dy_hbm, wg_hbm, wu_hbm, wd_hbm, ga, gb, P_, H, DY, AT, DT, ACC, HID, DG, DU, wg_v, wu_v, wd_v, *comm):
    (sb_a, keep_a, r1_a, s2_a, k2_a, r2_a, s3_a, acc_a, r3_a, s4_a, r4_a, g_a,
     sb_b, keep_b, r1_b, s2_b, acc1_b, r2_b, s3_b, k2_b, r3_b, s4_b, r4_b, g_b,
     load_sem, w_sem, loc_a, loc_b, first_send, first_recv, early_recv, send_a, send_b, *recvs) = comm
    recv_a = dict(zip(range(2, 8), recvs[:6], strict=True))
    recv_b = dict(zip(range(2, 8), recvs[6:], strict=True))
    me = lax.axis_index("dp")
    c = me % 2
    z = (me // 2) % 4
    y = me // 8
    odd = z % 2
    high = z // 2
    inner = (odd + high) == 1
    end = (odd + high) != 1
    to_core = me + 1 - 2 * c
    to_y = me + 8 - 16 * y
    to_z = me + 2 - 4 * odd
    to_mid = me + 2 - 4 * high

    def remote(src, dst, send, recv, to):
        return pltpu.make_async_remote_copy(
            src_ref=src, dst_ref=dst, send_sem=send, recv_sem=recv, device_id={"dp": to}, device_id_type=MESH
        )

    barrier = pltpu.get_barrier_semaphore()
    for to in (to_core, to_y, to_z):
        pl.semaphore_signal(barrier, inc=1, device_id={"dp": to}, device_id_type=MESH)

    @pl.when(inner)
    def _():
        pl.semaphore_signal(barrier, inc=1, device_id={"dp": to_mid}, device_id_type=MESH)
        pl.semaphore_wait(barrier, 4)

    @pl.when(end)
    def _():
        pl.semaphore_wait(barrier, 3)

    def weight_copies(i):
        layer, j, slot = (i // PER_LAYER) % 2, i % PER_LAYER, i % 2
        cols = pl.ds(pl.multiple_of(j * BLOCK, BLOCK), BLOCK)
        return (
            pltpu.make_async_copy(wg_hbm.at[layer, :, cols], wg_v.at[slot], w_sem.at[slot, 0]),
            pltpu.make_async_copy(wu_hbm.at[layer, :, cols], wu_v.at[slot], w_sem.at[slot, 1]),
            pltpu.make_async_copy(wd_hbm.at[layer, cols, :], wd_v.at[slot], w_sem.at[slot, 2]),
        )

    def fetch(i):
        for copy in weight_copies(i):
            copy.start()

    def arrive(i):
        for copy in weight_copies(i):
            copy.wait()

    fetch(0)
    loads = [
        pltpu.make_async_copy(x_hbm.at[0, k * TILE : (k + 1) * TILE], H.at[k * TILE : (k + 1) * TILE], load_sem.at[k])
        for k in range(TOKENS // TILE)
    ]
    load_dy = pltpu.make_async_copy(dy_hbm.at[0], DY, load_sem.at[TOKENS // TILE])
    for load in loads:
        load.start()
    load_dy.start()

    def tiles(body):
        for k in range(TOKENS // TILE):
            body(slice(k * TILE, (k + 1) * TILE))

    def normed(h):
        wide = h.astype(F32)
        return (wide * scale_of(wide)).astype(BF16)

    def down_of(a, slot):
        gate, up = nn(a, wg_v[slot]), nn(a, wu_v[slot])
        return nn((gate * jax.nn.sigmoid(gate) * up).astype(BF16), wd_v[slot])

    def flip_a_share(i):
        for k in range(TOKENS // TILE):
            q = pl.ds(pl.multiple_of((i * (TOKENS // TILE) + k) * LANES, LANES), LANES)
            AT[0, :, q] = P_[0, q, :].T
            DT[:, q] = DY[q, :].T

    def first(at):
        a = normed(H[at, :])
        P_[0, at, :] = a
        ACC[at, :] = down_of(a, 0)

    def last(at):
        total = ACC[at, :] + down_of(P_[0, at, :], (PER_LAYER - 1) % 2)
        h = (H[at, :].astype(F32) + total.astype(BF16).astype(F32)).astype(BF16)
        H[at, :] = h
        a = normed(h)
        P_[1, at, :] = a
        AT[1, :, at] = a.T
        ACC[at, :] = jnp.zeros((TILE, D), F32)

    def forward(i, flips):
        slot = i % 2
        arrive(i)
        fetch(i + 1)

        def body(at):
            ACC[at, :] += down_of(P_[0, at, :], slot)

        tiles(body)
        if flips:
            flip_a_share(i - 1)

    arrive(0)
    fetch(1)
    for k, load in enumerate(loads):
        load.wait()
        first(slice(k * TILE, (k + 1) * TILE))
    load_dy.wait()
    with_flips = 1 + TILE // LANES

    @pl.loop(1, with_flips)
    def _(i):
        forward(i, True)

    @pl.loop(with_flips, PER_LAYER - 1)
    def _(i):
        forward(i, False)

    arrive(PER_LAYER - 1)
    fetch(PER_LAYER)
    tiles(last)

    def own_a(b):
        return ga.at[b, :, rows(c * HALF + y * QUARTER, QUARTER), :]

    def other_a(b):
        return ga.at[b, :, rows(c * HALF + (1 - y) * QUARTER, QUARTER), :]

    def core_of(g, b, which):
        return g.at[b, :, rows(which * HALF, HALF), :]

    def own_b(b):
        return gb.at[b, :, rows(c * HALF + high * QUARTER, QUARTER), :]

    def other_b(b):
        return gb.at[b, :, rows(c * HALF + (1 - high) * QUARTER, QUARTER), :]

    def live(t, s):
        return (t - s >= 0) & (t - s < BLOCKS)

    def a_copy(s, b, src, dst, to):
        return remote(src, dst, send_a.at[s], recv_a[s].at[b % SLOTS_A[s]], to)

    def b_copy(s, b, src, dst, to):
        return remote(src, dst, send_b.at[s], recv_b[s].at[b % SLOTS_B[s]], to)

    def first_a(b, m):
        slot = b % 2
        return remote(sb_a.at[slot, m], r1_a.at[slot, m], first_send.at[0, slot, m], first_recv.at[0, slot, m], to_core)

    def first_b(b, m):
        slot = b % 2
        return remote(sb_b.at[slot, m], r1_b.at[slot, m], first_send.at[1, slot, m], first_recv.at[1, slot, m], to_core)

    def tick_a(t):
        @pl.when(live(t, 6))
        def _():
            b = t - 6
            a_copy(7, b, core_of(ga, b, c), core_of(ga, b, c), to_core).wait_send()
            a_copy(7, b, core_of(ga, b, 1 - c), core_of(ga, b, 1 - c), to_core).wait_recv()

        @pl.when(live(t, 5))
        def _():
            b = t - 5
            a_copy(6, b, own_a(b), own_a(b), to_y).wait_send()
            a_copy(6, b, other_a(b), other_a(b), to_y).wait_recv()
            a_copy(7, b, core_of(ga, b, c), core_of(ga, b, c), to_core).start()

        @pl.when(live(t, 4))
        def _():
            b = t - 4

            @pl.when(inner)
            def _():
                a_copy(5, b, g_a, own_a(b), to_z).wait_send()
                pltpu.make_async_copy(g_a, own_a(b), loc_a).wait()

            @pl.when(end)
            def _():
                a_copy(5, b, g_a, own_a(b), to_z).wait_recv()

            a_copy(6, b, own_a(b), own_a(b), to_y).start()

        @pl.when(live(t, 3) & inner)
        def _():
            b = t - 3
            copy = a_copy(4, b, s4_a, r4_a.at[b % 2], to_mid)
            copy.wait_send()
            copy.wait_recv()
            g_a[...] = (s4_a[...].astype(F32) + r4_a[b % 2].astype(F32)).astype(BF16)
            pltpu.make_async_copy(g_a, own_a(b), loc_a).start()
            a_copy(5, b, g_a, own_a(b), to_z).start()

        @pl.when(live(t, 2))
        def _():
            b = t - 2
            slot = b % SLOTS_A[3]
            copy = a_copy(3, b, s3_a, r3_a.at[slot], to_z)

            @pl.when(end)
            def _():
                copy.wait_send()

            @pl.when(inner)
            def _():
                copy.wait_recv()
                s4_a[...] = (acc_a[...] + r3_a[slot].astype(F32)).astype(BF16)
                a_copy(4, b, s4_a, r4_a.at[b % 2], to_mid).start()

        @pl.when(live(t, 1))
        def _():
            b = t - 1
            copy = a_copy(2, b, s2_a, r2_a.at[b % 2], to_y)
            copy.wait_send()
            copy.wait_recv()
            total = k2_a[...] + r2_a[b % 2].astype(F32)

            @pl.when(inner)
            def _():
                acc_a[...] = total

            @pl.when(end)
            def _():
                s3_a[...] = total.astype(BF16)
                a_copy(3, b, s3_a, r3_a.at[b % SLOTS_A[3]], to_z).start()

        @pl.when(live(t, 0))
        def _():
            b = t
            slot = b % 2
            for m in range(3):
                first_a(b, m).wait()
            mine, theirs = rows(y * QUARTER, QUARTER), rows((1 - y) * QUARTER, QUARTER)
            k2_a[...] = keep_a[slot, :, mine, :] + r1_a[slot, :, mine, :].astype(F32)
            s2_a[...] = (keep_a[slot, :, theirs, :] + r1_a[slot, :, theirs, :].astype(F32)).astype(BF16)
            a_copy(2, b, s2_a, r2_a.at[slot], to_y).start()

    def out_own(b):
        return remote(g_b, own_b(b), send_b.at[0], early_recv.at[b % SLOTS_B[6]], to_z)

    def out_other(b):
        return b_copy(6, b, other_b(b), other_b(b), to_z)

    def late_b(t):
        @pl.when(live(t, 6))
        def _():
            b = t - 6
            b_copy(7, b, core_of(gb, b, c), core_of(gb, b, c), to_core).wait_send()
            b_copy(7, b, core_of(gb, b, 1 - c), core_of(gb, b, 1 - c), to_core).wait_recv()

        @pl.when(live(t, 5))
        def _():
            b = t - 5

            @pl.when(inner)
            def _():
                out_other(b).wait_send()

            @pl.when(end)
            def _():
                out_own(b).wait_recv()
                out_other(b).wait_recv()

            b_copy(7, b, core_of(gb, b, c), core_of(gb, b, c), to_core).start()

        @pl.when(live(t, 4) & inner)
        def _():
            b = t - 4
            b_copy(5, b, g_b, own_b(b), to_mid).wait_send()
            b_copy(5, b, g_b, other_b(b), to_mid).wait_recv()
            out_other(b).start()
            pltpu.make_async_copy(g_b, own_b(b), loc_b).wait()

    def tick_b(t):
        @pl.when(live(t, 4) & inner)
        def _():
            out_own(t - 4).wait_send()

        @pl.when(live(t, 3) & inner)
        def _():
            b = t - 3
            copy = b_copy(4, b, s4_b, r4_b.at[b % 2], to_y)
            copy.wait_send()
            copy.wait_recv()
            g_b[...] = (s4_b[...].astype(F32) + r4_b[b % 2].astype(F32)).astype(BF16)
            pltpu.make_async_copy(g_b, own_b(b), loc_b).start()
            b_copy(5, b, g_b, own_b(b), to_mid).start()
            out_own(b).start()

        @pl.when(live(t, 2) & inner)
        def _():
            b = t - 2
            copy = b_copy(3, b, s3_b, r3_b.at[b % 2], to_mid)
            copy.wait_send()
            copy.wait_recv()
            s4_b[...] = (k2_b[...] + r3_b[b % 2].astype(F32)).astype(BF16)
            b_copy(4, b, s4_b, r4_b.at[b % 2], to_y).start()

        @pl.when(live(t, 1))
        def _():
            b = t - 1
            slot = b % SLOTS_B[2]
            copy = b_copy(2, b, s2_b, r2_b.at[slot], to_z)

            @pl.when(end)
            def _():
                copy.wait_send()

            @pl.when(inner)
            def _():
                copy.wait_recv()
                mine, theirs = rows(high * QUARTER, QUARTER), rows((1 - high) * QUARTER, QUARTER)
                k2_b[...] = acc1_b[:, mine, :] + r2_b[slot, :, mine, :].astype(F32)
                s3_b[...] = (acc1_b[:, theirs, :] + r2_b[slot, :, theirs, :].astype(F32)).astype(BF16)
                b_copy(3, b, s3_b, r3_b.at[b % 2], to_mid).start()

        @pl.when(live(t, 0))
        def _():
            b = t
            slot = b % 2
            for m in range(3):
                first_b(b, m).wait()
            total = keep_b[slot] + r1_b[slot].astype(F32)

            @pl.when(inner)
            def _():
                acc1_b[...] = total

            @pl.when(end)
            def _():
                s2_b[...] = total.astype(BF16)
                b_copy(2, b, s2_b, r2_b.at[b % SLOTS_B[2]], to_z).start()

    def turn(at, by_a):
        wide = H[at, :].astype(F32)
        scale = scale_of(wide)
        da = by_a.astype(BF16).astype(F32)
        along = jnp.sum(da * wide, -1, keepdims=True) * (scale * scale * scale) * (1.0 / D)
        by_h = (da * scale - wide * along).astype(BF16).astype(F32)
        by_y = (DY[at, :].astype(F32) + by_h).astype(BF16)
        DY[at, :] = by_y
        DT[:, at] = by_y.T

    def gradients(t):
        slot = (t + PER_LAYER) % 2
        layer = 1 - t // PER_LAYER

        def body(at):
            a = P_[layer, at, :]
            gate, up = nn(a, wg_v[slot]), nn(a, wu_v[slot])
            by_hid = nt(DY[at, :], wd_v[slot]).astype(BF16).astype(F32)
            sig = jax.nn.sigmoid(gate)
            act = gate * sig
            HID[at, :] = (act * up).astype(BF16)
            by_gate = (by_hid * up * (sig + act * (1.0 - sig))).astype(BF16)
            by_up = (by_hid * act).astype(BF16)
            DG[at, :] = by_gate
            DU[at, :] = by_up

        tiles(body)

    def by_input(t, then=None):
        slot = (t + PER_LAYER) % 2

        def body(at):
            total = ACC[at, :] + (nt(DG[at, :], wg_v[slot]) + nt(DU[at, :], wu_v[slot]))
            if then is None:
                ACC[at, :] = total
            else:
                then(at, total)

        tiles(body)

    def weights_of(t):
        slot = t % 2
        layer = 1 - t // PER_LAYER
        pairs = ((AT.at[layer], DG), (AT.at[layer], DU), (DT, HID))

        def send(m):
            first_a(t, m).start()
            first_b(t, m).start()

        for m, (left, right) in enumerate(pairs):
            total = nn(left[rows((1 - c) * HALF, HALF), :], right[...]).astype(BF16)
            sb_a[slot, m] = total[:, :LANES]
            sb_b[slot, m] = total[:, LANES:]
            if m:
                send(m - 1)
        for m, (left, right) in enumerate(pairs):
            total = nn(left[rows(c * HALF, HALF), :], right[...])
            keep_a[slot, m] = total[:, :LANES]
            keep_b[slot, m] = total[:, LANES:]
            if m == 0:
                send(2)

    def main(t, carry):
        @pl.when(t < BLOCKS)
        def _():
            arrive(t + PER_LAYER)

            @pl.when(t < BLOCKS - 1)
            def _():
                fetch(t + PER_LAYER + 1)

            gradients(t)

        tick_b(t - 1)

        @pl.when(t < BLOCKS)
        def _():
            weights_of(t)

        @pl.when(t < PER_LAYER - 1)
        def _():
            by_input(t)

        @pl.when(t == PER_LAYER - 1)
        def _():
            by_input(t, turn)

        late_b(t)
        tick_a(t)
        return carry

    lax.fori_loop(0, BLOCKS + 6, main, 0)


def summed_gradients(x, dy, wg, wu, wd):
    unit = lambda n, height, dtype: pltpu.VMEM((n, 3, height, LANES) if n else (3, height, LANES), dtype)
    scratch = [
        pltpu.VMEM((2, TOKENS, D), BF16),
        pltpu.VMEM((TOKENS, D), BF16),
        pltpu.VMEM((TOKENS, D), BF16),
        pltpu.VMEM((2, D, TOKENS), BF16),
        pltpu.VMEM((D, TOKENS), BF16),
        pltpu.VMEM((TOKENS, D), F32),
        pltpu.VMEM((TOKENS, BLOCK), BF16),
        pltpu.VMEM((TOKENS, BLOCK), BF16),
        pltpu.VMEM((TOKENS, BLOCK), BF16),
        pltpu.VMEM((2, D, BLOCK), BF16),
        pltpu.VMEM((2, D, BLOCK), BF16),
        pltpu.VMEM((2, BLOCK, D), BF16),
        unit(2, HALF, BF16), unit(2, HALF, F32), unit(2, HALF, BF16),
        unit(0, QUARTER, BF16), unit(0, QUARTER, F32), unit(2, QUARTER, BF16),
        unit(0, QUARTER, BF16), unit(0, QUARTER, F32), unit(SLOTS_A[3], QUARTER, BF16),
        unit(0, QUARTER, BF16), unit(2, QUARTER, BF16), unit(0, QUARTER, BF16),
        unit(2, HALF, BF16), unit(2, HALF, F32), unit(2, HALF, BF16),
        unit(0, HALF, BF16), unit(0, HALF, F32), unit(SLOTS_B[2], HALF, BF16),
        unit(0, QUARTER, BF16), unit(0, QUARTER, F32), unit(2, QUARTER, BF16),
        unit(0, QUARTER, BF16), unit(2, QUARTER, BF16), unit(0, QUARTER, BF16),
        pltpu.SemaphoreType.DMA((TOKENS // TILE + 1,)),
        pltpu.SemaphoreType.DMA((2, 3)),
        pltpu.SemaphoreType.DMA,
        pltpu.SemaphoreType.DMA,
        pltpu.SemaphoreType.DMA((2, 2, 3)),
        pltpu.SemaphoreType.DMA((2, 2, 3)),
        pltpu.SemaphoreType.DMA((SLOTS_B[6],)),
        pltpu.SemaphoreType.DMA((8,)),
        pltpu.SemaphoreType.DMA((8,)),
        *[pltpu.SemaphoreType.DMA((SLOTS_A[s],)) for s in range(2, 8)],
        *[pltpu.SemaphoreType.DMA((SLOTS_B[s],)) for s in range(2, 8)],
    ]
    out = jax.ShapeDtypeStruct((BLOCKS, 3, D, LANES), BF16)
    return pl.pallas_call(
        step_kernel,
        out_shape=(out, out),
        in_specs=[pl.BlockSpec(memory_space=pl.ANY)] * 5,
        out_specs=(pl.BlockSpec(memory_space=pl.ANY),) * 2,
        scratch_shapes=scratch,
        compiler_params=pltpu.CompilerParams(collective_id=0, has_side_effects=True, vmem_limit_bytes=62 * 2**20),
        name="gradients",
    )(x, dy, wg, wu, wd)


def adamw(w, m, v, g):
    m = 0.9 * m + 0.1 * g
    v = 0.95 * v + 0.05 * g * g
    step = m * lax.rsqrt(v + 1e-8) + 0.1 * w
    return (w - 0.02 * step).astype(BF16), m, v


def update_wide(*refs):
    ins, outs = (refs[:5], refs[5:10]), (refs[10:13], refs[13:])
    for (w_ref, m_ref, v_ref, ga_ref, gb_ref), (w_out, m_out, v_out) in zip(ins, outs, strict=True):
        for j in range(FF // LANES):
            at = slice(j * LANES, (j + 1) * LANES)
            g = (ga_ref, gb_ref)[j % 2][j // 2, 0].astype(F32)
            w_out[0, :, at], m_out[0, :, at], v_out[0, :, at] = adamw(
                w_ref[0, :, at].astype(F32), m_ref[0, :, at], v_ref[0, :, at], g
            )


TALL = BLOCK
WIDE = 112


def update_tall(w_ref, m_ref, v_ref, ga_ref, gb_ref, w_out, m_out, v_out):
    for k in range(TALL // LANES):
        at = slice(k * LANES, (k + 1) * LANES)
        g = (ga_ref, gb_ref)[k % 2][k // 2, 0].T.astype(F32)
        w_out[0, at], m_out[0, at], v_out[0, at] = adamw(w_ref[0, at].astype(F32), m_ref[0, at], v_ref[0, at], g)


def update_all(*refs):
    @pl.when(pl.program_id(1) < D // WIDE)
    def _():
        update_wide(*refs[:10], *refs[15:21])

    update_tall(*refs[10:15], *refs[21:])


def update(gate, up, down, ga, gb):
    last = D // WIDE - 1
    wide = pl.BlockSpec((1, WIDE, FF), lambda l, i: (l, jnp.minimum(i, last), 0))
    tall = pl.BlockSpec((1, TALL, D), lambda l, i: (l, i, 0))

    def g_wide(which):
        return pl.BlockSpec((PER_LAYER, 1, WIDE, LANES), lambda l, i: (1 - l, which, jnp.minimum(i, last), 0))

    g_tall = pl.BlockSpec((1, 1, D, LANES), lambda l, i: ((1 - l) * PER_LAYER + i, 2, 0, 0))
    new = pl.pallas_call(
        update_all,
        grid=(2, PER_LAYER),
        in_specs=[wide] * 3 + [g_wide(0)] * 2 + [wide] * 3 + [g_wide(1)] * 2 + [tall] * 3 + [g_tall] * 2,
        out_specs=[wide] * 6 + [tall] * 3,
        out_shape=[
            jax.ShapeDtypeStruct(w.shape, t) for w in (gate[0], up[0], down[0]) for t in (BF16, F32, F32)
        ],
        compiler_params=pltpu.CompilerParams(vmem_limit_bytes=60 * 2**20),
        name="update",
    )(*gate, ga, gb, *up, ga, gb, *down, ga, gb)
    return new[:3], new[3:6], new[6:]


def solution(mesh):
    def step(x, dy, *arrays):
        weights, m, v = (arrays[i : i + 3] for i in (0, 3, 6))
        ga, gb = summed_gradients(x, dy, *weights)
        gate, up, down = zip(weights, m, v, strict=True)
        new = update(gate, up, down, ga, gb)
        return tuple(one[which] for which in range(3) for one in new)

    return jax.shard_map(
        step,
        mesh=mesh,
        in_specs=(P(("rep", "dp"), None, None),) * 2 + (P(None, None, None),) * 9,
        out_specs=(P("rep", None, None),) * 9,
        check_vma=False,
    )
```
